16 devices in a mesh: dp: 1, ep: 16 (over x, y, z, core).
Axes of the slice: x: 2, y: 2, z: 2, core: 2. Of those that a mesh axis runs over, the one named last changes fastest.
Arguments:
- x: bfloat16 [1, 16, 256, 2048], P('dp', 'ep')
- expert: int32 [1, 16, 256, 2], P('dp', 'ep')
- slot: int32 [1, 16, 256, 2], P('dp', 'ep')
- gate: float32 [1, 16, 256, 2], P('dp', 'ep')
- w_gate: bfloat16 [16, 2048, 14336], P('ep')
- w_up: bfloat16 [16, 2048, 14336], P('ep')
- w_down: bfloat16 [16, 14336, 2048], P('ep')
Outputs:
- y: bfloat16 [1, 16, 256, 2048], P('dp', 'ep')
All inputs are finite; a program needn't handle non-finite values.
Results may differ from the reference program's by a relative error of at most 0.009.
Values are sent between devices in bfloat16 or wider.
A program may use at most 2 GiB of HBM per device.

```python
import jax
import jax.numpy as jnp

MEMBERS = 16
TOKENS = 256
D = 2048
FF = 14336
TOP = 2
EXPERTS = 16
SLOTS = 5 * TOKENS * TOP // (4 * EXPERTS)


def setup_inputs(seed: int = 0, part: int = 0) -> dict:
    own, k1, k2, k3, k4, k5, k6 = jax.random.split(jax.random.key(seed), 7)
    kx, ke, kl, kg = jax.random.split(jax.random.fold_in(own, part), 4)
    devices = (1, MEMBERS)
    place = jax.random.permutation(kl, jnp.arange(EXPERTS, dtype=jnp.uint32))
    slow = ((EXPERTS + (9 * place) % EXPERTS) << ((9 * place) // EXPERTS)) // EXPERTS
    wait = (jax.random.bits(ke, (*devices, TOKENS, EXPERTS), jnp.uint32) >> 10) * slow
    expert = jnp.argsort(wait, axis=-1)[..., :TOP].astype(jnp.int32)
    chosen = jax.nn.one_hot(expert, EXPERTS, dtype=jnp.int32)
    in_line = jnp.cumsum(chosen.reshape(*devices, TOKENS * TOP, EXPERTS), axis=2) - 1
    slot = jnp.sum(in_line.reshape(chosen.shape) * chosen, axis=-1)

    def one(key, rows, columns):
        return (jax.random.normal(key, (rows, columns), jnp.float32) * rows**-0.5).astype(jnp.bfloat16)

    def weights(key, rows, columns):
        return jax.lax.map(lambda k: one(k, rows, columns), jax.random.split(key, EXPERTS))

    return {
        "x": jax.random.normal(kx, (*devices, TOKENS, D), jnp.float32).astype(jnp.bfloat16),
        "expert": expert,
        "slot": slot,
        "gate": jax.nn.softmax(jax.random.normal(kg, expert.shape, jnp.float32)),
        "w_gate": weights(k1, D, FF),
        "w_up": weights(k2, D, FF),
        "w_down": weights(k3, FF, D),
    }


def einsum(form, a, b):
    return jnp.einsum(form, a.astype(jnp.float32), b.astype(jnp.float32))


def reference(x, expert, slot, gate, w_gate, w_up, w_down):
    to_expert = jax.nn.one_hot(expert, EXPERTS, dtype=jnp.bfloat16)
    to_slot = jax.nn.one_hot(slot, SLOTS, dtype=jnp.bfloat16)
    weighted = to_expert * gate[..., None].astype(jnp.bfloat16)
    dispatch = einsum("abtke,abtkc->abtec", to_expert, to_slot).astype(jnp.bfloat16)
    combine = einsum("abtke,abtkc->abtec", weighted, to_slot).astype(jnp.bfloat16)
    z = einsum("abtec,abtd->aebcd", dispatch, x).astype(jnp.bfloat16)
    h = jax.nn.silu(einsum("aebcd,edf->aebcf", z, w_gate))
    h = (h * einsum("aebcd,edf->aebcf", z, w_up)).astype(jnp.bfloat16)
    out = einsum("aebcf,efd->aebcd", h, w_down).astype(jnp.bfloat16)
    y = einsum("abtec,aebcd->abtd", combine, out)
    return y.astype(jnp.bfloat16)
```

```python
import functools

import jax
import jax.numpy as jnp
from jax import lax
from jax.experimental import pallas as pl
from jax.experimental.pallas import tpu as pltpu
from jax.sharding import PartitionSpec as P

MESH = pl.DeviceIdType.MESH
ORDER = (0, 1, 2, 4, 8, 3, 5, 9, 6, 10, 12, 7, 11, 13, 14, 15)
SENDS = ORDER[1:]
FAR_FIRST = tuple(reversed(SENDS))
NEAR = 8
FT = 512
NT = 256
BUFS = 3
COMM = True


def partner(me, mask):
    out = me
    for b in range(4):
        if mask >> b & 1:
            out = out + (1 << b) * (1 - 2 * ((me // (1 << b)) % 2))
    return out


def kernel(dims, x_hbm, expert_hbm, slot_hbm, gate_hbm, wg_hbm, wu_hbm, wd_hbm, y_ref,
           x, expert, slot, gate, z_send, z_recv, z, weight, h, wg, wu, wd, o_send, o_recv,
           in_sem, w_sem, d_sem, zs_sem, zr_sem, os_sem, or_sem):
    n, slots, tokens, d, ff = dims
    rows, near = n * slots, NEAR * slots
    f_tiles, n_tiles = ff // FT, d // NT
    me = lax.axis_index("ep")
    f32, bf16 = jnp.float32, jnp.bfloat16

    def device(mask):
        return {"ep": partner(me, mask)}

    ins = [pltpu.make_async_copy(a, b, in_sem.at[i]) for i, (a, b) in enumerate(
        ((x_hbm, x), (expert_hbm, expert), (slot_hbm, slot), (gate_hbm, gate)))]
    for c in ins:
        c.start()

    def fetch(i):
        columns = pl.ds(pl.multiple_of((i % f_tiles) * FT, FT), FT)
        s = i % BUFS
        return (pltpu.make_async_copy(wg_hbm.at[:, columns], wg.at[s], w_sem.at[0, s]),
                pltpu.make_async_copy(wu_hbm.at[:, columns], wu.at[s], w_sem.at[1, s]))

    def fetch_down(i):
        columns = pl.ds(pl.multiple_of(i * NT, NT), NT)
        return pltpu.make_async_copy(wd_hbm.at[:, columns], wd.at[i % 2], d_sem.at[i % 2])

    if COMM:
        barrier = pltpu.get_barrier_semaphore()
        for mask in SENDS:
            pl.semaphore_signal(barrier, inc=1, device_id=device(mask), device_id_type=MESH)

    for i in range(BUFS - 1):
        for c in fetch(i):
            c.start()

    for c in ins:
        c.wait()
    place = jnp.where(slot[...] < slots, (expert[...] ^ me) * slots + slot[...], -1)
    at = lax.broadcasted_iota(jnp.int32, (rows, tokens), 0)
    first, second = at == place[0:1, :], at == place[1:2, :]
    pick = jnp.where(first | second, 1.0, 0.0).astype(bf16)
    g = gate[...].astype(bf16).astype(f32)
    zero = jnp.zeros((rows, tokens), f32)
    weight[...] = (jnp.where(first, g[0:1, :], zero) + jnp.where(second, g[1:2, :], zero)).T.astype(bf16)
    sent = jnp.dot(pick, x[...], preferred_element_type=f32)
    for m in range(n):
        (z_recv if m == 0 else z_send)[m] = sent[m * slots:(m + 1) * slots].astype(bf16)

    def send_z(mask):
        return pltpu.make_async_remote_copy(
            src_ref=z_send.at[mask], dst_ref=z_recv.at[mask], send_sem=zs_sem.at[mask], recv_sem=zr_sem.at[mask],
            device_id=device(mask), device_id_type=MESH)

    if COMM:
        pl.semaphore_wait(barrier, n - 1)
        for mask in SENDS:
            send_z(mask).start()

    def settle(lo, hi):
        if COMM:
            for p in range(lo, hi):
                if ORDER[p]:
                    send_z(ORDER[p]).wait_recv()
        for p in range(lo, hi, 2):
            pair = [z_recv[ORDER[q]].astype(f32) for q in (p, p + 1)]
            z[p * slots:(p + 2) * slots, :] = jnp.concatenate(pair, axis=0).astype(bf16)

    def up(first_tile, last_tile, row, count):
        @pl.loop(first_tile, last_tile)
        def _(i):
            s = i % BUFS
            for c in fetch(i):
                c.wait()

            @pl.when(i + BUFS - 1 < 2 * f_tiles)
            def _():
                for c in fetch(i + BUFS - 1):
                    c.start()

            @pl.when(i == 2 * f_tiles - BUFS)
            def _():
                fetch_down(0).start()

            zz = z[row:row + count, :]
            a = jnp.dot(zz, wg[s], preferred_element_type=f32)
            b = jnp.dot(zz, wu[s], preferred_element_type=f32)
            columns = pl.ds(pl.multiple_of((i % f_tiles) * FT, FT), FT)
            h[row:row + count, columns] = (a * jax.nn.sigmoid(a) * b).astype(bf16)

    settle(0, NEAR)
    up(0, f_tiles, 0, near)
    settle(NEAR, n)
    up(f_tiles, 2 * f_tiles, near, rows - near)

    def send_o(t, mask):
        return pltpu.make_async_remote_copy(
            src_ref=o_send.at[t, mask], dst_ref=o_recv.at[t, mask], send_sem=os_sem.at[t], recv_sem=or_sem.at[t],
            device_id=device(mask), device_id_type=MESH)

    def combine(t):
        if COMM:
            arrived = o_recv.at[t, pl.ds(1, n - 1)]
            pltpu.make_async_copy(arrived, arrived, or_sem.at[t]).wait()
        back = jnp.concatenate([o_recv[t, m].astype(f32) for m in range(n)], axis=0).astype(bf16)
        y_ref[:, pl.ds(pl.multiple_of(t * NT, NT), NT)] = jnp.dot(
            weight[...], back, preferred_element_type=f32).astype(bf16)

    @pl.loop(0, n_tiles)
    def _(t):
        fetch_down(t).wait()

        @pl.when(t + 1 < n_tiles)
        def _():
            fetch_down(t + 1).start()

        o = jnp.dot(h[...], wd[t % 2], preferred_element_type=f32)
        for p in range(n):
            m = ORDER[p]
            (o_send if m else o_recv)[t, m] = o[p * slots:(p + 1) * slots].astype(bf16)
        if COMM:
            for mask in FAR_FIRST:
                send_o(t, mask).start()

        @pl.when(t >= 2)
        def _():
            combine(t - 2)

    for t in range(n_tiles - 2, n_tiles):
        combine(t)
    if COMM:
        for mask in SENDS:
            send_z(mask).wait_send()
        for t in range(n_tiles):
            left = o_send.at[t, pl.ds(1, n - 1)]
            pltpu.make_async_copy(left, left, os_sem.at[t]).wait()


def solution(mesh):
    n = mesh.shape["ep"]

    def local(x, expert, slot, gate, w_gate, w_up, w_down):
        _, d, ff = w_gate.shape
        tokens, top = expert.shape[2:]
        slots = 5 * tokens * top // (4 * n)
        rows = n * slots
        n_tiles = d // NT
        bf16 = jnp.bfloat16
        any_ = pl.BlockSpec(memory_space=pl.ANY)
        y = pl.pallas_call(
            functools.partial(kernel, (n, slots, tokens, d, ff)),
            out_shape=jax.ShapeDtypeStruct((tokens, d), bf16),
            in_specs=[any_] * 7,
            out_specs=pl.BlockSpec(memory_space=pltpu.VMEM),
            scratch_shapes=[
                pltpu.VMEM((tokens, d), bf16),
                pltpu.VMEM((top, tokens), jnp.int32),
                pltpu.VMEM((top, tokens), jnp.int32),
                pltpu.VMEM((top, tokens), jnp.float32),
                pltpu.VMEM((n, slots, d), bf16),
                pltpu.VMEM((n, slots, d), bf16),
                pltpu.VMEM((rows, d), bf16),
                pltpu.VMEM((tokens, rows), bf16),
                pltpu.VMEM((rows, ff), bf16),
                pltpu.VMEM((BUFS, d, FT), bf16),
                pltpu.VMEM((BUFS, d, FT), bf16),
                pltpu.VMEM((2, ff, NT), bf16),
                pltpu.VMEM((n_tiles, n, slots, NT), bf16),
                pltpu.VMEM((n_tiles, n, slots, NT), bf16),
                pltpu.SemaphoreType.DMA((4,)),
                pltpu.SemaphoreType.DMA((2, BUFS)),
                pltpu.SemaphoreType.DMA((2,)),
                pltpu.SemaphoreType.DMA((n,)),
                pltpu.SemaphoreType.DMA((n,)),
                pltpu.SemaphoreType.DMA((n_tiles,)),
                pltpu.SemaphoreType.DMA((n_tiles,)),
            ],
            compiler_params=pltpu.CompilerParams(
                vmem_limit_bytes=67043328,
                **(dict(collective_id=0, has_side_effects=True) if COMM else {})),
        )(x[0, 0], expert[0, 0].T, slot[0, 0].T, gate[0, 0].T, w_gate[0], w_up[0], w_down[0])
        return y[None, None]

    tok, exp = P("dp", "ep", None, None), P("ep", None, None)
    return jax.shard_map(local, mesh=mesh, in_specs=(tok,) * 4 + (exp,) * 3, out_specs=tok, check_vma=False)
```

```python
import functools

import jax
import jax.numpy as jnp
from jax import lax
from jax.experimental import pallas as pl
from jax.experimental.pallas import tpu as pltpu
from jax.sharding import PartitionSpec as P

MESH = pl.DeviceIdType.MESH
ORDER = (0, 1, 2, 4, 8, 3, 5, 9, 6, 10, 12, 7, 11, 13, 14, 15)
SENDS = ORDER[1:]
FAR_FIRST = tuple(reversed(SENDS))
NEAR = 8
FT = 512
NT = 256
PAIR = 2
RING = 3
EARLY = 8
LAG = 5
COMM = True


def partner(me, mask):
    out = me
    for b in range(4):
        if mask >> b & 1:
            out = out + (1 << b) * (1 - 2 * ((me // (1 << b)) % 2))
    return out


def kernel(dims, x_hbm, expert_hbm, slot_hbm, gate_hbm, wg_hbm, wu_hbm, wd_hbm, y_ref,
           x, expert, slot, gate, z_send, z_recv, z, weight, h, pool, o_send, o_recv,
           in_sem, w_sem, d_sem, zs_sem, zr_sem, os_sem, or_sem):
    n, slots, tokens, d, ff = dims
    rows, near = n * slots, NEAR * slots
    groups, n_tiles, chunks = ff // (FT * PAIR), d // NT, ff // d
    steps = groups + EARLY
    turn = (RING - steps) % RING
    me = lax.axis_index("ep")
    f32, bf16 = jnp.float32, jnp.bfloat16

    def device(mask):
        return {"ep": partner(me, mask)}

    if COMM:
        barrier = pltpu.get_barrier_semaphore()
        for mask in SENDS:
            pl.semaphore_signal(barrier, inc=1, device_id=device(mask), device_id_type=MESH)

    ins = [pltpu.make_async_copy(a, b, in_sem.at[i]) for i, (a, b) in enumerate(
        ((x_hbm, x), (expert_hbm, expert), (slot_hbm, slot), (gate_hbm, gate)))]
    for c in ins:
        c.start()

    def place_of(q, u):
        column = ((q % groups) * PAIR + u) * FT
        return 2 * (PAIR * ((q + turn) % RING) + u), pl.ds(pl.multiple_of(column, FT), FT)

    def fetch(q):
        copies = []
        for u in range(PAIR):
            s, columns = place_of(q, u)
            copies.append(pltpu.make_async_copy(wg_hbm.at[:, columns], pool.at[s], w_sem.at[s]))
            copies.append(pltpu.make_async_copy(wu_hbm.at[:, columns], pool.at[s + 1], w_sem.at[s + 1]))
        return copies

    def half(t):
        return pl.ds(pl.multiple_of((t % 2) * NT, NT), NT)

    def fetch_down(t, ks=None):
        columns = pl.ds(pl.multiple_of(t * NT, NT), NT)
        return [pltpu.make_async_copy(wd_hbm.at[pl.ds(k * d, d), columns], pool.at[k, :, half(t)], d_sem.at[t % 2, k])
                for k in (range(chunks) if ks is None else ks)]

    for c in fetch(0):
        c.start()

    for c in ins:
        c.wait()
    place = jnp.where(slot[...] < slots, (expert[...] ^ me) * slots + slot[...], -1)
    at = lax.broadcasted_iota(jnp.int32, (rows, tokens), 0)
    first, second = at == place[0:1, :], at == place[1:2, :]
    pick = jnp.where(first | second, 1.0, 0.0).astype(bf16)
    g = gate[...].astype(bf16).astype(f32)
    zero = jnp.zeros((rows, tokens), f32)
    weight[...] = (jnp.where(first, g[0:1, :], zero) + jnp.where(second, g[1:2, :], zero)).T.astype(bf16)
    sent = jnp.dot(pick, x[...], preferred_element_type=f32)
    for m in range(n):
        (z_recv if m == 0 else z_send)[m] = sent[m * slots:(m + 1) * slots].astype(bf16)

    def send_z(mask):
        return pltpu.make_async_remote_copy(
            src_ref=z_send.at[mask], dst_ref=z_recv.at[mask], send_sem=zs_sem.at[mask], recv_sem=zr_sem.at[mask],
            device_id=device(mask), device_id_type=MESH)

    if COMM:
        pl.semaphore_wait(barrier, n - 1)
        for mask in SENDS:
            send_z(mask).start()
    for q in range(1, RING):
        for c in fetch(q):
            c.start()

    def settle(lo, hi):
        if COMM:
            for p in range(lo, hi):
                if ORDER[p]:
                    send_z(ORDER[p]).wait_recv()
        for p in range(lo, hi, 2):
            pair = [z_recv[ORDER[q]].astype(f32) for q in (p, p + 1)]
            z[p * slots:(p + 2) * slots, :] = jnp.concatenate(pair, axis=0).astype(bf16)

    def up(q, row, count):
        rows_ = z[row:row + count, :]
        for u in range(PAIR):
            s, columns = place_of(q, u)
            a = jnp.dot(rows_, pool[s], preferred_element_type=f32)
            b = jnp.dot(rows_, pool[s + 1], preferred_element_type=f32)
            h[row:row + count, columns] = (a * jax.nn.sigmoid(a) * b).astype(bf16)

    def ready(q):
        for c in fetch(q):
            c.wait()

    def refill(q):
        @pl.when(q + RING - 1 < steps)
        def _():
            for c in fetch(q + RING - 1):
                c.start()

    settle(0, 4)

    @pl.loop(0, RING)
    def _(q):
        ready(q)
        up(q, 0, near // 2)

    settle(4, NEAR)

    @pl.loop(0, RING)
    def _(q):
        @pl.when(q > 0)
        def _():
            refill(q)

        up(q, near // 2, near // 2)

    @pl.loop(RING, EARLY)
    def _(q):
        ready(q)
        refill(q)
        up(q, 0, near)

    settle(NEAR, n)

    @pl.loop(EARLY, groups)
    def _(q):
        ready(q)
        refill(q)
        up(q, 0, rows)

    split = 2 * PAIR

    @pl.loop(groups, steps)
    def _(q):
        ready(q)
        refill(q)

        @pl.when(q == steps - 2)
        def _():
            for c in fetch_down(0, range(split)):
                c.start()

        @pl.when(q == steps - 1)
        def _():
            for c in fetch_down(0, range(split, chunks)) + fetch_down(1):
                c.start()

        up(q, near, rows - near)

    def send_o(t, mask):
        return pltpu.make_async_remote_copy(
            src_ref=o_send.at[t, mask], dst_ref=o_recv.at[t, mask], send_sem=os_sem.at[t], recv_sem=or_sem.at[t],
            device_id=device(mask), device_id_type=MESH)

    def combine(t):
        for u in (t, t + 1):
            if COMM:
                arrived = o_recv.at[u, pl.ds(1, n - 1)]
                pltpu.make_async_copy(arrived, arrived, or_sem.at[u]).wait()
        for u in (t, t + 1):
            back = jnp.concatenate([o_recv[u, m].astype(f32) for m in range(n)], axis=0).astype(bf16)
            y_ref[:, pl.ds(pl.multiple_of(u * NT, NT), NT)] = jnp.dot(
                weight[...], back, preferred_element_type=f32).astype(bf16)

    @pl.loop(0, n_tiles)
    def _(t):
        for c in fetch_down(t):
            c.wait()

        @pl.when((t >= 1) & (t + 1 < n_tiles))
        def _():
            for c in fetch_down(t + 1):
                c.start()

        w = pool[0:chunks, :, half(t)].reshape(ff, NT)
        o = jnp.dot(h[...], w, preferred_element_type=f32)
        for p in range(n):
            m = ORDER[p]
            (o_send if m else o_recv)[t, m] = o[p * slots:(p + 1) * slots].astype(bf16)
        if COMM:
            for mask in FAR_FIRST:
                send_o(t, mask).start()

        @pl.when((t >= LAG) & (t % 2 == LAG % 2))
        def _():
            combine(t - LAG)

    for t in range((n_tiles - LAG + 1) // 2 * 2, n_tiles, 2):
        combine(t)
    if COMM:
        for mask in SENDS:
            send_z(mask).wait_send()
        for t in range(n_tiles):
            left = o_send.at[t, pl.ds(1, n - 1)]
            pltpu.make_async_copy(left, left, os_sem.at[t]).wait()


def solution(mesh):
    n = mesh.shape["ep"]

    def local(x, expert, slot, gate, w_gate, w_up, w_down):
        _, d, ff = w_gate.shape
        tokens, top = expert.shape[2:]
        slots = 5 * tokens * top // (4 * n)
        rows = n * slots
        n_tiles = d // NT
        bf16 = jnp.bfloat16
        any_ = pl.BlockSpec(memory_space=pl.ANY)
        y = pl.pallas_call(
            functools.partial(kernel, (n, slots, tokens, d, ff)),
            out_shape=pltpu.VMEM((tokens, d), bf16),
            in_specs=[any_] * 7,
            out_specs=pl.BlockSpec(memory_space=pltpu.VMEM),
            scratch_shapes=[
                pltpu.VMEM((tokens, d), bf16),
                pltpu.VMEM((top, tokens), jnp.int32),
                pltpu.VMEM((top, tokens), jnp.int32),
                pltpu.VMEM((top, tokens), jnp.float32),
                pltpu.VMEM((n, slots, d), bf16),
                pltpu.VMEM((n, slots, d), bf16),
                pltpu.VMEM((rows, d), bf16),
                pltpu.VMEM((tokens, rows), bf16),
                pltpu.VMEM((rows, ff), bf16),
                pltpu.VMEM((2 * PAIR * RING, d, FT), bf16),
                pltpu.VMEM((n_tiles, n, slots, NT), bf16),
                pltpu.VMEM((n_tiles, n, slots, NT), bf16),
                pltpu.SemaphoreType.DMA((4,)),
                pltpu.SemaphoreType.DMA((2 * PAIR * RING,)),
                pltpu.SemaphoreType.DMA((2, ff // d)),
                pltpu.SemaphoreType.DMA((n,)),
                pltpu.SemaphoreType.DMA((n,)),
                pltpu.SemaphoreType.DMA((n_tiles,)),
                pltpu.SemaphoreType.DMA((n_tiles,)),
            ],
            compiler_params=pltpu.CompilerParams(
                vmem_limit_bytes=67043328 - 2 * tokens * d - (1 << 16),
                **(dict(collective_id=0, has_side_effects=True) if COMM else {})),
        )(x[0, 0], expert[0, 0].T, slot[0, 0].T, gate[0, 0].T, w_gate[0], w_up[0], w_down[0])
        return y[None, None]

    tok, exp = P("dp", "ep", None, None), P("ep", None, None)
    return jax.shard_map(local, mesh=mesh, in_specs=(tok,) * 4 + (exp,) * 3, out_specs=tok, check_vma=False)
```

```python
import functools

import jax
import jax.numpy as jnp
from jax import lax
from jax.experimental import pallas as pl
from jax.experimental.pallas import tpu as pltpu
from jax.sharding import PartitionSpec as P

MESH = pl.DeviceIdType.MESH
ORDER = (0, 1, 2, 4, 8, 3, 5, 9, 6, 10, 12, 7, 11, 13, 14, 15)
SENDS = ORDER[1:]
FAR_FIRST = tuple(reversed(SENDS))
NEAR = 8
FT = 512
NT = 256
PAIR = 2
RING = 3
EARLY = 10
LAG = 5
COMM = True


def partner(me, mask):
    out = me
    for b in range(4):
        if mask >> b & 1:
            out = out + (1 << b) * (1 - 2 * ((me // (1 << b)) % 2))
    return out


def kernel(dims, x_hbm, expert_hbm, slot_hbm, gate_hbm, wg_hbm, wu_hbm, wd_hbm, y_ref,
           x, expert, slot, gate, z_send, z_recv, z, weight, h, pool, o_send, o_recv,
           in_sem, w_sem, d_sem, zs_sem, zr_sem, os_sem, or_sem):
    n, slots, tokens, d, ff = dims
    rows, near = n * slots, NEAR * slots
    groups, n_tiles, chunks = ff // (FT * PAIR), d // NT, ff // d
    steps = groups + EARLY
    turn = (RING - steps) % RING
    me = lax.axis_index("ep")
    f32, bf16 = jnp.float32, jnp.bfloat16

    def device(mask):
        return {"ep": partner(me, mask)}

    if COMM:
        barrier = pltpu.get_barrier_semaphore()
        for mask in SENDS:
            pl.semaphore_signal(barrier, inc=1, device_id=device(mask), device_id_type=MESH)

    ins = [pltpu.make_async_copy(a, b, in_sem.at[i]) for i, (a, b) in enumerate(
        ((x_hbm, x), (expert_hbm, expert), (slot_hbm, slot), (gate_hbm, gate)))]
    for c in ins:
        c.start()

    def place_of(q, u):
        column = ((q % groups) * PAIR + u) * FT
        return 2 * (PAIR * ((q + turn) % RING) + u), pl.ds(pl.multiple_of(column, FT), FT)

    def fetch(q):
        copies = []
        for u in range(PAIR):
            s, columns = place_of(q, u)
            copies.append(pltpu.make_async_copy(wg_hbm.at[:, columns], pool.at[s], w_sem.at[s]))
            copies.append(pltpu.make_async_copy(wu_hbm.at[:, columns], pool.at[s + 1], w_sem.at[s + 1]))
        return copies

    def half(t):
        return pl.ds(pl.multiple_of((t % 2) * NT, NT), NT)

    def fetch_down(t, ks=None):
        columns = pl.ds(pl.multiple_of(t * NT, NT), NT)
        return [pltpu.make_async_copy(wd_hbm.at[pl.ds(k * d, d), columns], pool.at[k, :, half(t)], d_sem.at[t % 2, k])
                for k in (range(chunks) if ks is None else ks)]

    for c in fetch(0):
        c.start()

    for c in ins:
        c.wait()
    place = jnp.where(slot[...] < slots, (expert[...] ^ me) * slots + slot[...], -1)
    at = lax.broadcasted_iota(jnp.int32, (rows, tokens), 0)
    first, second = at == place[0:1, :], at == place[1:2, :]
    pick = jnp.where(first | second, 1.0, 0.0).astype(bf16)
    g = gate[...].astype(bf16).astype(f32)
    zero = jnp.zeros((rows, tokens), f32)
    weight[...] = (jnp.where(first, g[0:1, :], zero) + jnp.where(second, g[1:2, :], zero)).T.astype(bf16)
    sent = jnp.dot(pick, x[...], preferred_element_type=f32)
    for m in range(n):
        (z_recv if m == 0 else z_send)[m] = sent[m * slots:(m + 1) * slots].astype(bf16)

    def send_z(mask):
        return pltpu.make_async_remote_copy(
            src_ref=z_send.at[mask], dst_ref=z_recv.at[mask], send_sem=zs_sem.at[mask], recv_sem=zr_sem.at[mask],
            device_id=device(mask), device_id_type=MESH)

    if COMM:
        pl.semaphore_wait(barrier, n - 1)
        for mask in ORDER[1:NEAR]:
            send_z(mask).start()
    for q in range(1, RING):
        for c in fetch(q):
            c.start()

    def settle(lo, hi):
        if COMM:
            for p in range(lo, hi):
                if ORDER[p]:
                    send_z(ORDER[p]).wait_recv()
        for p in range(lo, hi, 2):
            pair = [z_recv[ORDER[q]].astype(f32) for q in (p, p + 1)]
            z[p * slots:(p + 2) * slots, :] = jnp.concatenate(pair, axis=0).astype(bf16)

    def up(q, row, count):
        rows_ = z[row:row + count, :]
        for u in range(PAIR):
            s, columns = place_of(q, u)
            a = jnp.dot(rows_, pool[s], preferred_element_type=f32)
            b = jnp.dot(rows_, pool[s + 1], preferred_element_type=f32)
            h[row:row + count, columns] = (a * jax.nn.sigmoid(a) * b).astype(bf16)

    def ready(q):
        for c in fetch(q):
            c.wait()

    def refill(q):
        @pl.when(q + RING - 1 < steps)
        def _():
            for c in fetch(q + RING - 1):
                c.start()

    settle(0, 4)

    @pl.loop(0, RING)
    def _(q):
        ready(q)
        up(q, 0, near // 2)

    if COMM:
        for mask in ORDER[NEAR:]:
            send_z(mask).start()

    settle(4, NEAR)

    @pl.loop(0, RING)
    def _(q):
        @pl.when(q > 0)
        def _():
            refill(q)

        up(q, near // 2, near // 2)

    @pl.loop(RING, EARLY)
    def _(q):
        ready(q)
        refill(q)
        up(q, 0, near)

    settle(NEAR, n)

    @pl.loop(EARLY, groups)
    def _(q):
        ready(q)
        refill(q)
        up(q, 0, rows)

    split = 2 * PAIR

    @pl.loop(groups, steps)
    def _(q):
        ready(q)
        refill(q)

        @pl.when(q == steps - 2)
        def _():
            for c in fetch_down(0, range(split)):
                c.start()

        @pl.when(q == steps - 1)
        def _():
            for c in fetch_down(0, range(split, chunks)) + fetch_down(1):
                c.start()

        up(q, near, rows - near)

    def send_o(t, mask):
        return pltpu.make_async_remote_copy(
            src_ref=o_send.at[t, mask], dst_ref=o_recv.at[t, mask], send_sem=os_sem.at[t], recv_sem=or_sem.at[t],
            device_id=device(mask), device_id_type=MESH)

    def combine(t):
        for u in (t, t + 1):
            if COMM:
                arrived = o_recv.at[u, pl.ds(1, n - 1)]
                pltpu.make_async_copy(arrived, arrived, or_sem.at[u]).wait()
        for u in (t, t + 1):
            back = jnp.concatenate([o_recv[u, m].astype(f32) for m in range(n)], axis=0).astype(bf16)
            y_ref[:, pl.ds(pl.multiple_of(u * NT, NT), NT)] = jnp.dot(
                weight[...], back, preferred_element_type=f32).astype(bf16)

    @pl.loop(0, n_tiles)
    def _(t):
        for c in fetch_down(t):
            c.wait()

        @pl.when((t >= 1) & (t + 1 < n_tiles))
        def _():
            for c in fetch_down(t + 1):
                c.start()

        w = pool[0:chunks, :, half(t)].reshape(ff, NT)
        o = jnp.dot(h[...], w, preferred_element_type=f32)
        for p in range(n):
            m = ORDER[p]
            (o_send if m else o_recv)[t, m] = o[p * slots:(p + 1) * slots].astype(bf16)
        if COMM:
            for mask in FAR_FIRST:
                send_o(t, mask).start()

        @pl.when((t >= LAG) & (t % 2 == LAG % 2))
        def _():
            combine(t - LAG)

    for t in range((n_tiles - LAG + 1) // 2 * 2, n_tiles, 2):
        combine(t)
    if COMM:
        for mask in SENDS:
            send_z(mask).wait_send()
        for t in range(n_tiles):
            left = o_send.at[t, pl.ds(1, n - 1)]
            pltpu.make_async_copy(left, left, os_sem.at[t]).wait()


def solution(mesh):
    n = mesh.shape["ep"]

    def local(x, expert, slot, gate, w_gate, w_up, w_down):
        _, d, ff = w_gate.shape
        tokens, top = expert.shape[2:]
        slots = 5 * tokens * top // (4 * n)
        rows = n * slots
        n_tiles = d // NT
        bf16 = jnp.bfloat16
        any_ = pl.BlockSpec(memory_space=pl.ANY)
        y = pl.pallas_call(
            functools.partial(kernel, (n, slots, tokens, d, ff)),
            out_shape=pltpu.VMEM((tokens, d), bf16),
            in_specs=[any_] * 7,
            out_specs=pl.BlockSpec(memory_space=pltpu.VMEM),
            scratch_shapes=[
                pltpu.VMEM((tokens, d), bf16),
                pltpu.VMEM((top, tokens), jnp.int32),
                pltpu.VMEM((top, tokens), jnp.int32),
                pltpu.VMEM((top, tokens), jnp.float32),
                pltpu.VMEM((n, slots, d), bf16),
                pltpu.VMEM((n, slots, d), bf16),
                pltpu.VMEM((rows, d), bf16),
                pltpu.VMEM((tokens, rows), bf16),
                pltpu.VMEM((rows, ff), bf16),
                pltpu.VMEM((2 * PAIR * RING, d, FT), bf16),
                pltpu.VMEM((n_tiles, n, slots, NT), bf16),
                pltpu.VMEM((n_tiles, n, slots, NT), bf16),
                pltpu.SemaphoreType.DMA((4,)),
                pltpu.SemaphoreType.DMA((2 * PAIR * RING,)),
                pltpu.SemaphoreType.DMA((2, ff // d)),
                pltpu.SemaphoreType.DMA((n,)),
                pltpu.SemaphoreType.DMA((n,)),
                pltpu.SemaphoreType.DMA((n_tiles,)),
                pltpu.SemaphoreType.DMA((n_tiles,)),
            ],
            compiler_params=pltpu.CompilerParams(
                vmem_limit_bytes=67043328 - 2 * tokens * d - (1 << 16),
                **(dict(collective_id=0, has_side_effects=True) if COMM else {})),
        )(x[0, 0], expert[0, 0].T, slot[0, 0].T, gate[0, 0].T, w_gate[0], w_up[0], w_down[0])
        return y[None, None]

    tok, exp = P("dp", "ep", None, None), P("ep", None, None)
    return jax.shard_map(local, mesh=mesh, in_specs=(tok,) * 4 + (exp,) * 3, out_specs=tok, check_vma=False)
```

```python
import functools

import jax
import jax.numpy as jnp
from jax import lax
from jax.experimental import pallas as pl
from jax.experimental.pallas import tpu as pltpu
from jax.sharding import PartitionSpec as P

MESH = pl.DeviceIdType.MESH
ORDER = (0, 1, 2, 4, 8, 3, 5, 9, 6, 10, 12, 7, 11, 13, 14, 15)
SENDS = ORDER[1:]
FAR_FIRST = tuple(reversed(SENDS))
NEAR = 8
FT = 512
NT = 256
PAIR = 2
RING = 3
EARLY = 10
COMM = True


def partner(me, mask):
    out = me
    for b in range(4):
        if mask >> b & 1:
            out = out + (1 << b) * (1 - 2 * ((me // (1 << b)) % 2))
    return out


def kernel(dims, x_hbm, expert_hbm, slot_hbm, gate_hbm, wg_hbm, wu_hbm, wd_hbm, y_ref,
           x, expert, slot, gate, z_send, z_recv, z, weight, h, pool, o_send, o_recv,
           in_sem, w_sem, d_sem, zs_sem, zr_sem, os_sem, or_sem):
    n, slots, tokens, d, ff = dims
    rows, near = n * slots, NEAR * slots
    groups, n_tiles, chunks = ff // (FT * PAIR), d // NT, ff // d
    steps = groups + EARLY
    turn = (RING - steps) % RING
    me = lax.axis_index("ep")
    f32, bf16 = jnp.float32, jnp.bfloat16

    def device(mask):
        return {"ep": partner(me, mask)}

    if COMM:
        barrier = pltpu.get_barrier_semaphore()
        for mask in SENDS:
            pl.semaphore_signal(barrier, inc=1, device_id=device(mask), device_id_type=MESH)

    ins = [pltpu.make_async_copy(a, b, in_sem.at[i]) for i, (a, b) in enumerate(
        ((x_hbm, x), (expert_hbm, expert), (slot_hbm, slot), (gate_hbm, gate)))]
    for c in ins:
        c.start()

    def place_of(q, u):
        column = ((q % groups) * PAIR + u) * FT
        return 2 * (PAIR * ((q + turn) % RING) + u), pl.ds(pl.multiple_of(column, FT), FT)

    def fetch(q):
        copies = []
        for u in range(PAIR):
            s, columns = place_of(q, u)
            copies.append(pltpu.make_async_copy(wg_hbm.at[:, columns], pool.at[s], w_sem.at[s]))
            copies.append(pltpu.make_async_copy(wu_hbm.at[:, columns], pool.at[s + 1], w_sem.at[s + 1]))
        return copies

    def half(t):
        return pl.ds(pl.multiple_of((t % 2) * NT, NT), NT)

    def fetch_down(t, ks=None):
        columns = pl.ds(pl.multiple_of(t * NT, NT), NT)
        return [pltpu.make_async_copy(wd_hbm.at[pl.ds(k * d, d), columns], pool.at[k, :, half(t)], d_sem.at[t % 2, k])
                for k in (range(chunks) if ks is None else ks)]

    for c in fetch(0):
        c.start()

    for c in ins:
        c.wait()
    place = jnp.where(slot[...] < slots, (expert[...] ^ me) * slots + slot[...], -1)
    at = lax.broadcasted_iota(jnp.int32, (rows, tokens), 0)
    first, second = at == place[0:1, :], at == place[1:2, :]
    pick = jnp.where(first | second, 1.0, 0.0).astype(bf16)
    g = gate[...].astype(bf16).astype(f32)
    zero = jnp.zeros((rows, tokens), f32)
    weight[...] = (jnp.where(first, g[0:1, :], zero) + jnp.where(second, g[1:2, :], zero)).T.astype(bf16)
    sent = jnp.dot(pick, x[...], preferred_element_type=f32)
    for m in range(n):
        (z_recv if m == 0 else z_send)[m] = sent[m * slots:(m + 1) * slots].astype(bf16)

    def send_z(mask):
        return pltpu.make_async_remote_copy(
            src_ref=z_send.at[mask], dst_ref=z_recv.at[mask], send_sem=zs_sem.at[mask], recv_sem=zr_sem.at[mask],
            device_id=device(mask), device_id_type=MESH)

    if COMM:
        pl.semaphore_wait(barrier, n - 1)
        for mask in ORDER[1:NEAR]:
            send_z(mask).start()
    for q in range(1, RING):
        for c in fetch(q):
            c.start()

    def settle(lo, hi):
        if COMM:
            for p in range(lo, hi):
                if ORDER[p]:
                    send_z(ORDER[p]).wait_recv()
        for p in range(lo, hi, 2):
            pair = [z_recv[ORDER[q]].astype(f32) for q in (p, p + 1)]
            z[p * slots:(p + 2) * slots, :] = jnp.concatenate(pair, axis=0).astype(bf16)

    def up(q, row, count):
        rows_ = z[row:row + count, :]
        for u in range(PAIR):
            s, columns = place_of(q, u)
            a = jnp.dot(rows_, pool[s], preferred_element_type=f32)
            b = jnp.dot(rows_, pool[s + 1], preferred_element_type=f32)
            h[row:row + count, columns] = (a * jax.nn.sigmoid(a) * b).astype(bf16)

    def ready(q):
        for c in fetch(q):
            c.wait()

    def refill(q):
        @pl.when(q + RING - 1 < steps)
        def _():
            for c in fetch(q + RING - 1):
                c.start()

    settle(0, 4)

    @pl.loop(0, RING)
    def _(q):
        ready(q)
        up(q, 0, near // 2)

    if COMM:
        for mask in ORDER[NEAR:]:
            send_z(mask).start()

    settle(4, NEAR)

    @pl.loop(0, RING)
    def _(q):
        @pl.when(q > 0)
        def _():
            refill(q)

        up(q, near // 2, near // 2)

    @pl.loop(RING, EARLY)
    def _(q):
        ready(q)
        refill(q)
        up(q, 0, near)

    settle(NEAR, n)

    @pl.loop(EARLY, groups)
    def _(q):
        ready(q)
        refill(q)
        up(q, 0, rows)

    split = 2 * PAIR

    @pl.loop(groups, steps)
    def _(q):
        ready(q)
        refill(q)

        @pl.when(q == steps - 2)
        def _():
            for c in fetch_down(0, range(split)):
                c.start()

        @pl.when(q == steps - 1)
        def _():
            for c in fetch_down(0, range(split, chunks)) + fetch_down(1):
                c.start()

        up(q, near, rows - near)

    def send_o(t, mask):
        return pltpu.make_async_remote_copy(
            src_ref=o_send.at[t, mask], dst_ref=o_recv.at[t, mask], send_sem=os_sem.at[t], recv_sem=or_sem.at[t],
            device_id=device(mask), device_id_type=MESH)

    def combine(t):
        if COMM:
            arrived = o_recv.at[t, pl.ds(1, n - 1)]
            pltpu.make_async_copy(arrived, arrived, or_sem.at[t]).wait()
        back = jnp.concatenate([o_recv[t, m].astype(f32) for m in range(n)], axis=0).astype(bf16)
        y_ref[:, pl.ds(pl.multiple_of(t * NT, NT), NT)] = jnp.dot(
            weight[...], back, preferred_element_type=f32).astype(bf16)

    @pl.loop(0, n_tiles)
    def _(t):
        for c in fetch_down(t):
            c.wait()

        @pl.when((t >= 1) & (t + 1 < n_tiles))
        def _():
            for c in fetch_down(t + 1):
                c.start()

        w = pool[0:chunks, :, half(t)].reshape(ff, NT)
        o = jnp.dot(h[...], w, preferred_element_type=f32)
        for p in range(n):
            m = ORDER[p]
            (o_send if m else o_recv)[t, m] = o[p * slots:(p + 1) * slots].astype(bf16)
        if COMM:
            for mask in FAR_FIRST:
                send_o(t, mask).start()

    @pl.loop(0, n_tiles)
    def _(t):
        combine(t)

    if COMM:
        for mask in SENDS:
            send_z(mask).wait_send()
        for t in range(n_tiles):
            left = o_send.at[t, pl.ds(1, n - 1)]
            pltpu.make_async_copy(left, left, os_sem.at[t]).wait()


def solution(mesh):
    n = mesh.shape["ep"]

    def local(x, expert, slot, gate, w_gate, w_up, w_down):
        _, d, ff = w_gate.shape
        tokens, top = expert.shape[2:]
        slots = 5 * tokens * top // (4 * n)
        rows = n * slots
        n_tiles = d // NT
        bf16 = jnp.bfloat16
        any_ = pl.BlockSpec(memory_space=pl.ANY)
        y = pl.pallas_call(
            functools.partial(kernel, (n, slots, tokens, d, ff)),
            out_shape=pltpu.VMEM((tokens, d), bf16),
            in_specs=[any_] * 7,
            out_specs=pl.BlockSpec(memory_space=pltpu.VMEM),
            scratch_shapes=[
                pltpu.VMEM((tokens, d), bf16),
                pltpu.VMEM((top, tokens), jnp.int32),
                pltpu.VMEM((top, tokens), jnp.int32),
                pltpu.VMEM((top, tokens), jnp.float32),
                pltpu.VMEM((n, slots, d), bf16),
                pltpu.VMEM((n, slots, d), bf16),
                pltpu.VMEM((rows, d), bf16),
                pltpu.VMEM((tokens, rows), bf16),
                pltpu.VMEM((rows, ff), bf16),
                pltpu.VMEM((2 * PAIR * RING, d, FT), bf16),
                pltpu.VMEM((n_tiles, n, slots, NT), bf16),
                pltpu.VMEM((n_tiles, n, slots, NT), bf16),
                pltpu.SemaphoreType.DMA((4,)),
                pltpu.SemaphoreType.DMA((2 * PAIR * RING,)),
                pltpu.SemaphoreType.DMA((2, ff // d)),
                pltpu.SemaphoreType.DMA((n,)),
                pltpu.SemaphoreType.DMA((n,)),
                pltpu.SemaphoreType.DMA((n_tiles,)),
                pltpu.SemaphoreType.DMA((n_tiles,)),
            ],
            compiler_params=pltpu.CompilerParams(
                vmem_limit_bytes=67043328 - 2 * tokens * d - (1 << 16),
                **(dict(collective_id=0, has_side_effects=True) if COMM else {})),
        )(x[0, 0], expert[0, 0].T, slot[0, 0].T, gate[0, 0].T, w_gate[0], w_up[0], w_down[0])
        return y[None, None]

    tok, exp = P("dp", "ep", None, None), P("ep", None, None)
    return jax.shard_map(local, mesh=mesh, in_specs=(tok,) * 4 + (exp,) * 3, out_specs=tok, check_vma=False)
```
